32 devices in a mesh: seq: 8 (over z, core), head: 4 (over y, x).
Axes of the slice: x: 2, y: 2, z: 4, core: 2. Of those that a mesh axis runs over, the one named last changes fastest.
Arguments:
- grid_state: bfloat16 [65536, 1024], P('seq', 'head'), may hold values from -6 to 6
- encode_index: int32 [128, 8], P('seq'), may hold values from 0 to 511, as said below
- encode_weights: bfloat16 [128, 8, 128, 128], P('seq'), may hold values from -0.1875 to 0.1875
- first_gain: float32 [1024], replicated, may hold values from 0.1 to 1.9
- project_in: bfloat16 [1024, 3, 1024], P(None, None, 'head'), may hold values from -8 to 8
- project_out: bfloat16 [1024, 1024], P('head'), may hold values from -0.25 to 0.25
- second_gain: float32 [1024], replicated, may hold values from 0.1 to 1.9
- expand_weights: bfloat16 [1024, 4096], P(None, 'head'), may hold values from -0.1875 to 0.1875
- shrink_weights: bfloat16 [4096, 1024], P('head'), may hold values from -0.125 to 0.125
- decode_index: int32 [512, 2], P('seq'), may hold values from 0 to 127, as said below
- decode_weights: bfloat16 [512, 2, 128, 128], P('seq'), may hold values from -0.375 to 0.375
- output_gain: float32 [1024], P('head'), may hold values from 0.1 to 1.9
Outputs:
- grid_output: bfloat16 [65536, 1024], P('seq', 'head')
The draws below stay inside these ranges and needn't reach their ends.
Inputs may be any that keep to these rules, and one draw needn't show every extreme that they name: `encode_index`: for a mesh block of band b (blocks b * 16 onward), every entry lies in b * 64 - 2048 / 128 to (b + 1) * 64 + 2048 / 128 - 1. `decode_index`: for a grid block of band b (blocks b * 64 onward), every entry lies in b * 16 - 2048 / 256 to (b + 1) * 16 + 2048 / 256 - 1, with the division rounded down.
All inputs are finite; a program needn't handle non-finite values.
Results may differ from the reference program's by a relative error of at most 0.012.
Values may be sent and summed in bfloat16 or wider, within the bound.
A program may use at most 128 MiB of HBM per device.

```python
import jax
import jax.numpy as jnp
from jax import lax

D = 1024
HEADS = 16
MLP = 4096
HEAD_DIM = 64
WINDOW = 1120
M_DEV = 2048
G_DEV = 8192
BLOCK = 128
SLOTS_IN = 8
SLOTS_OUT = 2
GRID = 65536
MESH_BLOCKS = 128
GRID_BLOCKS = 512


def band_table(key, row_count, rows_band, rim_blocks, own_blocks, total_blocks, slot_count):
    row_iota = jnp.arange(row_count, dtype=jnp.int32)
    band_number = row_iota // rows_band
    lowest = jnp.maximum(band_number * own_blocks - rim_blocks, 0)
    highest = jnp.minimum((band_number + 1) * own_blocks + rim_blocks, total_blocks)
    drawn = jax.random.randint(key, (row_count, slot_count), lowest[:, None], highest[:, None])
    within = row_iota % rows_band
    drawn = drawn.at[:, 0].set(jnp.where(within == 0, lowest, drawn[:, 0]))
    drawn = drawn.at[:, slot_count - 1].set(jnp.where(within == rows_band - 1, highest - 1, drawn[:, slot_count - 1]))
    return drawn.astype(jnp.int32)


def draw_encode_index(key, part):
    mesh_band = M_DEV // BLOCK
    return band_table(jax.random.fold_in(key, 11), MESH_BLOCKS, mesh_band, mesh_band, G_DEV // BLOCK, GRID_BLOCKS, SLOTS_IN)


def draw_decode_index(key, part):
    mesh_band = M_DEV // BLOCK
    return band_table(jax.random.fold_in(key, 13), GRID_BLOCKS, G_DEV // BLOCK, mesh_band // 2, mesh_band, MESH_BLOCKS, SLOTS_OUT)


def draw_project_in(key, part):
    matrix = jax.random.normal(jax.random.fold_in(key, 17), (D, 3, D), jnp.float32) * D ** (-0.5)
    return jnp.clip(matrix, -8.0, 8.0).astype(jnp.bfloat16)


def strengthened(array, key, source, target, parts, factor):
    owner, partner = [(jnp.arange(array.shape[dim]) // (array.shape[dim] // parts)).reshape([-1 if axis == dim else 1 for axis in range(array.ndim)]) for dim in (source, target)]
    chosen = jax.random.permutation(key, parts)[partner]
    strong = (owner == chosen) | (owner == (partner + parts // 2) % parts)
    return jnp.where(strong, factor * array, array)


def level_of(stream_key, shape, pieces, least, high):
    def one(dim, blocks):
        steps = jax.random.uniform(jax.random.fold_in(jax.random.fold_in(stream_key, 6), dim), (blocks,), jnp.float32, least / len(pieces), high / len(pieces))
        return jnp.repeat(jnp.exp(steps), shape[dim] // blocks).reshape((-1,) + (1,) * (len(shape) - dim - 1))

    factor_of = one(*pieces[0])
    for cut in pieces[1:]:
        factor_of = factor_of * one(*cut)
    return factor_of


def bell_draw(key, extent, scale, limit, split=(), held_as=jnp.bfloat16):
    level = level_of(key, extent, split, -0.22, 0.18) if split else 1.0
    result = jax.random.normal(key, extent, jnp.float32) * scale * level
    return jnp.minimum(jnp.maximum(result, -limit), limit).astype(held_as)


def heavy_noise(own_key, shape, scale, bound, cuts, heavy, kind=jnp.bfloat16):
    result = scale * jax.random.normal(own_key, shape, jnp.float32)
    if cuts:
        result = result * level_of(own_key, shape, cuts, -0.22, 0.18)
    return jnp.clip(strengthened(result, jax.random.fold_in(own_key, 3), *heavy), -bound, bound).astype(kind)


def setup_inputs(seed: int = 0) -> dict:
    key_of = jax.random.split(jax.random.key(seed), 13)
    return {
        "grid_state": bell_draw(key_of[0], (GRID, D), 1.0, 6.0, ((0, 8), (1, 4))),
        "encode_index": draw_encode_index(jax.random.fold_in(key_of[12], 71), 0),
        "encode_weights": bell_draw(key_of[2], (MESH_BLOCKS, SLOTS_IN, BLOCK, BLOCK), (SLOTS_IN * BLOCK) ** -0.5, 0.1875, ((0, 8),)),
        "first_gain": jnp.clip(1.0 + 0.18 * jax.random.normal(key_of[3], (D,), jnp.float32), 0.1, 1.9),
        "project_in": draw_project_in(jax.random.fold_in(key_of[12], 71), 0),
        "project_out": heavy_noise(key_of[5], (D, D), D ** -0.5, 0.25, ((0, 4),), (0, 1, 4, 2.0)),
        "second_gain": jnp.clip(1.0 + 0.18 * jax.random.normal(key_of[6], (D,), jnp.float32), 0.1, 1.9),
        "expand_weights": bell_draw(key_of[7], (D, MLP), D ** -0.5, 0.1875, ((1, 4),)),
        "shrink_weights": heavy_noise(key_of[8], (MLP, D), MLP ** -0.5, 0.125, ((0, 4),), (0, 1, 4, 2.0)),
        "decode_index": draw_decode_index(jax.random.fold_in(key_of[12], 71), 0),
        "decode_weights": bell_draw(key_of[10], (GRID_BLOCKS, SLOTS_OUT, BLOCK, BLOCK), (SLOTS_OUT * BLOCK) ** -0.5, 0.375, ((0, 8),)),
        "output_gain": jnp.clip(1.0 + 0.18 * jax.random.normal(key_of[11], (D,), jnp.float32), 0.1, 1.9),
    }


EPSILON = 1e-05

def settle(values):
    return lax.optimization_barrier(values)

def layer_norm(values, scales):
    average = lax.optimization_barrier(jnp.mean(values, axis=1, keepdims=True))
    centred = values - average
    spread = lax.optimization_barrier(jnp.mean(centred * centred, axis=1, keepdims=True))
    return centred * lax.rsqrt(spread + EPSILON) * scales

def interpolate(source, index_table, weight_table):
    columns = source.shape[1]
    blocks = source.reshape(-1, BLOCK, columns)

    def one_block(pair):
        position, weight_block = pair
        picked = jnp.take(blocks, position, axis=0).astype(jnp.float32)
        return jnp.einsum('kij,kjc->ic', weight_block.astype(jnp.float32), picked, precision=lax.Precision.HIGHEST)
    return lax.map(one_block, (index_table, weight_table)).reshape(-1, columns)

def window_mask(query_rows, key_count, key_anchor, total_rows):
    query_iota = lax.broadcasted_iota(jnp.int32, (query_rows, key_count), 0)
    key_iota = lax.broadcasted_iota(jnp.int32, (query_rows, key_count), 1)
    distance = key_iota - query_iota
    global_key = key_anchor + key_iota
    return (distance >= 0) & (distance <= 2 * WINDOW) & (global_key >= 0) & (global_key < total_rows)

def softmax_values(scores, allowed, value_block):
    masked = jnp.where(allowed[None], scores, -1e+30)
    highest = lax.optimization_barrier(jnp.max(masked, axis=2, keepdims=True))
    powers = jnp.where(allowed[None], jnp.exp(masked - highest), 0.0)
    probs = settle((powers / lax.optimization_barrier(jnp.sum(powers, axis=2, keepdims=True))).astype(jnp.bfloat16))
    context = jnp.einsum('hqk,khd->qhd', probs.astype(jnp.float32), value_block, precision=lax.Precision.HIGHEST)
    return context.astype(jnp.bfloat16)

def attention(queries, keys, values):
    total_rows = queries.shape[0]
    query_rows = min(512, M_DEV)
    key_count = query_rows + 2 * WINDOW
    padding = ((WINDOW, WINDOW), (0, 0), (0, 0))
    keys_wide = jnp.pad(keys, padding)
    values_wide = jnp.pad(values, padding)

    def attend(first_row):
        query_block = lax.dynamic_slice_in_dim(queries, first_row, query_rows, 0).astype(jnp.float32)
        key_block = lax.dynamic_slice_in_dim(keys_wide, first_row, key_count, 0).astype(jnp.float32)
        value_block = lax.dynamic_slice_in_dim(values_wide, first_row, key_count, 0).astype(jnp.float32)
        scores = jnp.einsum('qhd,khd->hqk', query_block, key_block, precision=lax.Precision.HIGHEST) * HEAD_DIM ** (-0.5)
        allowed = window_mask(query_rows, key_count, first_row - WINDOW, total_rows)
        return softmax_values(scores, allowed, value_block)
    starts = jnp.arange(total_rows // query_rows, dtype=jnp.int32) * query_rows
    return lax.map(attend, starts).reshape(total_rows, HEADS * HEAD_DIM)

def reference(grid_state, encode_index, encode_weights, first_gain, project_in, project_out, second_gain, expand_weights, shrink_weights, decode_index, decode_weights, output_gain):
    mesh_start = settle(interpolate(grid_state, encode_index, encode_weights).astype(jnp.bfloat16))
    first_norm = layer_norm(mesh_start.astype(jnp.float32), first_gain).astype(jnp.bfloat16)
    heads_shape = (mesh_start.shape[0], HEADS, HEAD_DIM)
    queries = settle(jnp.dot(first_norm, project_in[:, 0, :], preferred_element_type=jnp.float32).astype(jnp.bfloat16)).reshape(heads_shape)
    keys = settle(jnp.dot(first_norm, project_in[:, 1, :], preferred_element_type=jnp.float32).astype(jnp.bfloat16)).reshape(heads_shape)
    values = settle(jnp.dot(first_norm, project_in[:, 2, :], preferred_element_type=jnp.float32).astype(jnp.bfloat16)).reshape(heads_shape)
    context = attention(queries, keys, values)
    attended = jnp.dot(context, project_out, preferred_element_type=jnp.float32)
    mesh_middle = settle((mesh_start.astype(jnp.float32) + attended).astype(jnp.bfloat16))
    second_norm = layer_norm(mesh_middle.astype(jnp.float32), second_gain).astype(jnp.bfloat16)
    hidden = jax.nn.gelu(jnp.dot(second_norm, expand_weights, preferred_element_type=jnp.float32)).astype(jnp.bfloat16)
    shrunk = jnp.dot(hidden, shrink_weights, preferred_element_type=jnp.float32)
    mesh_end = settle((mesh_middle.astype(jnp.float32) + shrunk).astype(jnp.bfloat16))
    back = interpolate(mesh_end, decode_index, decode_weights)
    average = lax.optimization_barrier(jnp.sum(back, axis=1, keepdims=True)) / D
    squares = lax.optimization_barrier(jnp.sum(back * back, axis=1, keepdims=True)) / D
    normed = (back - average) * lax.rsqrt(squares - average * average + EPSILON) * output_gain
    return (grid_state.astype(jnp.float32) + normed).astype(jnp.bfloat16)
```

```python
import functools

import jax
import jax.numpy as jnp
from jax import lax
from jax.experimental import pallas as pl
from jax.experimental.pallas import tpu as pltpu
from jax.sharding import PartitionSpec as P

D = 1024
HEAD_DIM = 64
WINDOW = 1120
EPSILON = 1e-05
NEGATIVE = -1e30
Q_TILE = 256
K_CHUNK = 512
F32 = jnp.float32
BF16 = jnp.bfloat16
MIB = 1024 * 1024


def params(mib=48, dims=None):
    return pltpu.CompilerParams(vmem_limit_bytes=mib * MIB, dimension_semantics=dims)


def cost(flops, moved):
    return pl.CostEstimate(flops=int(flops), bytes_accessed=int(moved), transcendentals=0)


def rims(cells, width):
    count = lax.axis_size("seq")
    up = [(i, i + 1) for i in range(count - 1)]
    down = [(i + 1, i) for i in range(count - 1)]
    lower = lax.ppermute(cells[cells.shape[0] - width :], "seq", up)
    upper = lax.ppermute(cells[:width], "seq", down)
    return lower, upper


def flipped(value, bit):
    count = lax.axis_size("head")
    return lax.ppermute(value, "head", [(i, i ^ bit) for i in range(count)])


def everyone(value):
    count = lax.axis_size("head")
    if count != 4:
        return [value] + [flipped(value, j) for j in range(1, count)]
    half = value.shape[0] // 2
    first = flipped(value, 1)
    second = flipped(value, 2)
    third = jnp.concatenate([flipped(first[:half], 2), flipped(second[half:], 1)], axis=0)
    return [value, first, second, third]


def load_wide(parts, wide, sems):
    copies = []
    at = 0
    for number, part in enumerate(parts):
        rows = part.shape[0]
        copies.append(pltpu.make_async_copy(part, wide.at[pl.ds(at, rows)], sems.at[number]))
        at += rows
    for copy in copies:
        copy.start()
    for copy in copies:
        copy.wait()


def gathered_dot(table, weights, wide, block, local, slots):
    rows = weights.shape[2]
    picked = []
    for k in range(slots):
        at = pl.multiple_of(table[block * slots + k] * rows, rows)
        picked.append(wide[pl.ds(at, rows), :])
    left = jnp.concatenate([weights[local, k] for k in range(slots)], axis=1)
    return left, jnp.concatenate(picked, axis=0)


def encode_kernel(per_step, table, low, own, high, weights, out, wide, sems):
    step = pl.program_id(0)

    @pl.when(step == 0)
    def _():
        load_wide((low, own, high), wide, sems)

    slots, rows = weights.shape[1], weights.shape[2]
    for local in range(per_step):
        left, right = gathered_dot(table, weights, wide, step * per_step + local, local, slots)
        out[local * rows : (local + 1) * rows, :] = jnp.dot(
            left, right, preferred_element_type=F32
        ).astype(BF16)


def encode(table, low, own, high, weights):
    blocks, slots, rows, _ = weights.shape
    columns = own.shape[1]
    per_step = 4
    wide_rows = low.shape[0] + own.shape[0] + high.shape[0]
    any_spec = pl.BlockSpec(memory_space=pl.ANY)
    return pl.pallas_call(
        functools.partial(encode_kernel, per_step),
        out_shape=jax.ShapeDtypeStruct((blocks * rows, columns), BF16),
        grid_spec=pltpu.PrefetchScalarGridSpec(
            num_scalar_prefetch=1,
            grid=(blocks // per_step,),
            in_specs=[any_spec] * 3
            + [pl.BlockSpec((per_step, slots, rows, rows), lambda i, t: (i, 0, 0, 0))],
            out_specs=pl.BlockSpec((per_step * rows, columns), lambda i, t: (i, 0)),
            scratch_shapes=[
                pltpu.VMEM((wide_rows, columns), BF16),
                pltpu.SemaphoreType.DMA((3,)),
            ],
        ),
        compiler_params=params(60, ("arbitrary",)),
        cost_estimate=cost(2 * blocks * slots * rows * rows * columns, wide_rows * columns * 2),
        name="encode",
    )(table, low, own, high, weights)


def project_kernel(count, order, *refs):
    pieces = refs[:count]
    gain, weight_q, weight_kv, out_q, out_kv = refs[count:]
    values = [p[...].astype(F32) for p in pieces]
    average = sum(jnp.sum(v, axis=1, keepdims=True) for v in values) / D
    centred = [v - average for v in values]
    spread = sum(jnp.sum(c * c, axis=1, keepdims=True) for c in centred) / D
    scale = lax.rsqrt(spread + EPSILON)
    queries, others = 0.0, 0.0
    for j in range(count):
        owner = order[j]
        normed = (centred[j] * scale * gain[owner]).astype(BF16)
        queries += jnp.dot(normed, weight_q[owner], preferred_element_type=F32)
        others += jnp.dot(normed, weight_kv[owner], preferred_element_type=F32)
    out_q[...] = (queries.astype(BF16).astype(F32) * HEAD_DIM ** (-0.5)).astype(BF16)
    out_kv[...] = others.astype(BF16)


def project(order, pieces, gain, weight_q, weight_kv):
    rows, columns = pieces[0].shape
    count = len(pieces)
    tile = 256
    whole = lambda *shape: pl.BlockSpec(shape, lambda i, t: (0,) * len(shape))
    return pl.pallas_call(
        functools.partial(project_kernel, count),
        out_shape=[
            jax.ShapeDtypeStruct((rows, columns), BF16),
            jax.ShapeDtypeStruct((rows, 2 * columns), BF16),
        ],
        grid_spec=pltpu.PrefetchScalarGridSpec(
            num_scalar_prefetch=1,
            grid=(rows // tile,),
            in_specs=[pl.BlockSpec((tile, columns), lambda i, t: (i, 0))] * count
            + [
                whole(count, 1, columns),
                whole(count, columns, columns),
                whole(count, columns, 2 * columns),
            ],
            out_specs=[
                pl.BlockSpec((tile, columns), lambda i, t: (i, 0)),
                pl.BlockSpec((tile, 2 * columns), lambda i, t: (i, 0)),
            ],
        ),
        compiler_params=params(60, ("arbitrary",)),
        cost_estimate=cost(6 * rows * D * columns, rows * D * 2),
        name="project",
    )(order, *pieces, gain, weight_q, weight_kv)


def attend_kernel(total, place, queries, low, own, high, out, wide, scores, masks):
    tile_number = pl.program_id(1)
    rim = low.shape[0]
    rows = own.shape[0]
    width = scores.shape[2]
    chunks = width // K_CHUNK

    @pl.when(tile_number == 0)
    def _():
        for a in range(2):
            lanes = slice(128 * a, 128 * (a + 1))
            wide[a, 0:rim, :] = low[:, lanes]
            wide[a, rim : rim + rows, :] = own[:, lanes]
            wide[a, rim + rows : 2 * rim + rows, :] = high[:, lanes]
            end = wide.shape[1] - (2 * rim + rows)
            wide[a, 2 * rim + rows :, :] = jnp.zeros((end, 128), BF16)
        q_iota = lax.broadcasted_iota(jnp.int32, (Q_TILE, K_CHUNK), 0)
        k_iota = lax.broadcasted_iota(jnp.int32, (Q_TILE, K_CHUNK), 1)
        for n, c in enumerate((0, chunks - 1)):
            distance = k_iota + c * K_CHUNK - q_iota
            allowed = (distance >= 0) & (distance <= 2 * WINDOW)
            masks[n] = jnp.where(allowed, 0.0, NEGATIVE)

    start = pl.multiple_of(tile_number * Q_TILE, Q_TILE)
    anchor = place[0] - WINDOW + start
    lane = lax.broadcasted_iota(jnp.int32, (Q_TILE, 128), 1)
    peaks = []
    for a in range(2):
        here = (lane < HEAD_DIM) if a == 0 else (lane >= HEAD_DIM)
        query = jnp.where(here, queries[...].astype(F32), 0.0).astype(BF16)
        peak = None
        for c in range(chunks):
            key = wide[a, pl.ds(start + c * K_CHUNK, K_CHUNK), :]
            score = lax.dot_general(
                query, key, (((1,), (1,)), ((), ())), preferred_element_type=F32
            )
            number = anchor + c * K_CHUNK + lax.broadcasted_iota(jnp.int32, (1, K_CHUNK), 1)
            score += jnp.where((number >= 0) & (number < total), 0.0, NEGATIVE)
            if c == 0:
                score += masks[0]
            if c == chunks - 1:
                score += masks[1]
            scores[a, :, c * K_CHUNK : (c + 1) * K_CHUNK] = score
            for part in range(K_CHUNK // 128):
                piece = score[:, part * 128 : (part + 1) * 128]
                peak = piece if peak is None else jnp.maximum(peak, piece)
        peaks.append(jnp.max(peak, axis=1, keepdims=True))
    results = []
    for a in range(2):
        gathered, weight = 0.0, 0.0
        for c in range(chunks):
            power = jnp.exp(scores[a, :, c * K_CHUNK : (c + 1) * K_CHUNK] - peaks[a])
            for part in range(K_CHUNK // 128):
                weight += power[:, part * 128 : (part + 1) * 128]
            value = wide[a, pl.ds(start + c * K_CHUNK, K_CHUNK), :]
            gathered += jnp.dot(power.astype(BF16), value, preferred_element_type=F32)
        results.append(gathered / jnp.sum(weight, axis=1, keepdims=True))
    out[...] = jnp.concatenate(
        [results[0][:, HEAD_DIM:], results[1][:, :HEAD_DIM]], axis=1
    ).astype(BF16)


def attend(place, total, queries, low, own, high):
    rows, columns = queries.shape
    rim = low.shape[0]
    width = -(-(Q_TILE + 2 * WINDOW) // K_CHUNK) * K_CHUNK
    wide_rows = rows - Q_TILE + width
    return pl.pallas_call(
        functools.partial(attend_kernel, total),
        out_shape=jax.ShapeDtypeStruct((rows, columns), BF16),
        grid_spec=pltpu.PrefetchScalarGridSpec(
            num_scalar_prefetch=1,
            grid=(columns // 128, rows // Q_TILE),
            in_specs=[
                pl.BlockSpec((Q_TILE, 128), lambda g, i, t: (i, g)),
                pl.BlockSpec((rim, 256), lambda g, i, t: (0, g)),
                pl.BlockSpec((rows, 256), lambda g, i, t: (0, g)),
                pl.BlockSpec((rim, 256), lambda g, i, t: (0, g)),
            ],
            out_specs=pl.BlockSpec((Q_TILE, 128), lambda g, i, t: (i, g)),
            scratch_shapes=[
                pltpu.VMEM((2, wide_rows, 128), BF16),
                pltpu.VMEM((2, Q_TILE, width), F32),
                pltpu.VMEM((2, Q_TILE, K_CHUNK), F32),
            ],
        ),
        compiler_params=params(60, ("arbitrary", "arbitrary")),
        cost_estimate=cost(16 * rows * width * columns, rows * columns * 8),
        name="attend",
    )(place, queries, low, own, high)


def feed_kernel(plan, units, *refs):
    context, start, gain, project_out = refs[:4]
    sources = refs[4:-6]
    out, normed, total, expand, shrink, sems = refs[-6:]
    width = start.shape[1]

    def copies(number):
        slot = number % 2
        made = []
        for source, rows, lanes, kind, at, to in plan[number]:
            buffer = expand if kind == "expand" else shrink
            taken = sources[source].at[pl.ds(rows[0], rows[1]), pl.ds(lanes[0], lanes[1])]
            placed = buffer.at[slot, pl.ds(at, rows[1]), pl.ds(to, lanes[1])]
            made.append(pltpu.make_async_copy(taken, placed, sems.at[slot, len(made)]))
        return made

    waiting = copies(0)
    for copy in waiting:
        copy.start()
    attended = jnp.dot(context[...], project_out[...], preferred_element_type=F32)
    middle = (start[...].astype(F32) + attended).astype(BF16).astype(F32)
    total[...] = middle
    average = jnp.mean(middle, axis=1, keepdims=True)
    centred = middle - average
    spread = jnp.mean(centred * centred, axis=1, keepdims=True)
    normed[...] = (centred * lax.rsqrt(spread + EPSILON) * gain[...]).astype(BF16)
    for number in range(len(plan)):
        for copy in waiting:
            copy.wait()
        if number + 1 < len(plan):
            waiting = copies(number + 1)
            for copy in waiting:
                copy.start()
        slot = number % 2
        wide = jnp.dot(normed[...], expand[slot], preferred_element_type=F32)
        hidden = jax.nn.gelu(wide).astype(BF16)
        total[...] += jnp.dot(hidden, shrink[slot], preferred_element_type=F32)
    out[...] = total[...].astype(BF16)


def whole_entry(source, base, units, width):
    cuts = width // units
    entry = [(source[0], (source[1], width), (0, units), "expand", 0, 0)]
    for c in range(cuts):
        entry.append((base[0], (base[1] + c * units, units), (0, units), "shrink", 0, c * units))
    return entry


def feed(context, start, gain, project_out, expand, shrink, packs):
    rows, width = start.shape
    units = expand.shape[1] // 2
    sources = [expand, shrink]
    plan = []
    for half in range(2):
        plan.append(
            [
                (0, (0, width), (half * units, units), "expand", 0, 0),
                (1, (half * units, units), (0, width), "shrink", 0, 0),
            ]
        )
    for pack in packs:
        at = len(sources)
        sources.extend(pack)
        if len(pack) == 1:
            plan.append(whole_entry((at, 0), (at, width), units, width))
        else:
            plan.append(whole_entry((at, 0), (at + 1, 0), units, width))
    vmem = pl.BlockSpec(memory_space=pltpu.VMEM)
    hbm = pl.BlockSpec(memory_space=pl.ANY)
    return pl.pallas_call(
        functools.partial(feed_kernel, plan, units),
        out_shape=jax.ShapeDtypeStruct((rows, width), BF16),
        in_specs=[vmem] * 4 + [hbm] * len(sources),
        out_specs=vmem,
        scratch_shapes=[
            pltpu.VMEM((rows, width), BF16),
            pltpu.VMEM((rows, width), F32),
            pltpu.VMEM((2, width, units), BF16),
            pltpu.VMEM((2, units, width), BF16),
            pltpu.SemaphoreType.DMA((2, 1 + width // units)),
        ],
        compiler_params=params(60),
        cost_estimate=cost(4 * rows * width * units * len(plan), 4 * width * units * len(plan)),
        name="feed",
    )(context, start, gain, project_out, *sources)


def sums_kernel(per_step, table, low, own, high, weights, out, wide, sems):
    step = pl.program_id(0)

    @pl.when(step == 0)
    def _():
        load_wide((low, own, high), wide, sems)

    slots = weights.shape[1]
    for local in range(per_step):
        left, right = gathered_dot(table, weights, wide, step * per_step + local, local, slots)
        back = lax.dot_general(right, left, (((0,), (1,)), ((), ())), preferred_element_type=F32)
        out[0, local : local + 1, :] = jnp.sum(back, axis=0, keepdims=True)
        out[1, local : local + 1, :] = jnp.sum(back * back, axis=0, keepdims=True)


def final_kernel(per_step, table, low, own, high, weights, sums, state, gain, out, wide, sems):
    step = pl.program_id(0)

    @pl.when(step == 0)
    def _():
        load_wide((low, own, high), wide, sems)

    average = sums[0] / D
    scale = lax.rsqrt(sums[1] / D - average * average + EPSILON)
    average = average.T
    scale = scale.T
    slots, rows = weights.shape[1], weights.shape[2]
    for local in range(per_step):
        left, right = gathered_dot(table, weights, wide, step * per_step + local, local, slots)
        back = jnp.dot(left, right, preferred_element_type=F32)
        normed = (back - average[:, local : local + 1]) * scale[:, local : local + 1] * gain[...]
        here = slice(local * rows, (local + 1) * rows)
        out[here, :] = (state[here, :].astype(F32) + normed).astype(BF16)


def decode_specs(low, own, high, weights, per_step):
    _, slots, rows, _ = weights.shape
    wide_rows = low.shape[0] + own.shape[0] + high.shape[0]
    ins = [pl.BlockSpec(memory_space=pl.ANY)] * 3 + [
        pl.BlockSpec((per_step, slots, rows, rows), lambda i, t: (i, 0, 0, 0))
    ]
    scratch = [pltpu.VMEM((wide_rows, own.shape[1]), BF16), pltpu.SemaphoreType.DMA((3,))]
    return ins, scratch


def decode_sums(table, low, own, high, weights):
    blocks, slots, rows, _ = weights.shape
    per_step = 8
    ins, scratch = decode_specs(low, own, high, weights, per_step)
    return pl.pallas_call(
        functools.partial(sums_kernel, per_step),
        out_shape=jax.ShapeDtypeStruct((2, blocks, rows), F32),
        grid_spec=pltpu.PrefetchScalarGridSpec(
            num_scalar_prefetch=1,
            grid=(blocks // per_step,),
            in_specs=ins,
            out_specs=pl.BlockSpec((2, per_step, rows), lambda i, t: (0, i, 0)),
            scratch_shapes=scratch,
        ),
        compiler_params=params(60, ("arbitrary",)),
        name="decode_sums",
    )(table, low, own, high, weights)


def decode_final(table, low, own, high, weights, sums, state, gain):
    blocks, slots, rows, _ = weights.shape
    columns = own.shape[1]
    per_step = 8
    ins, scratch = decode_specs(low, own, high, weights, per_step)
    return pl.pallas_call(
        functools.partial(final_kernel, per_step),
        out_shape=jax.ShapeDtypeStruct(state.shape, BF16),
        grid_spec=pltpu.PrefetchScalarGridSpec(
            num_scalar_prefetch=1,
            grid=(blocks // per_step,),
            in_specs=ins
            + [
                pl.BlockSpec((2, per_step, rows), lambda i, t: (0, i, 0)),
                pl.BlockSpec((per_step * rows, columns), lambda i, t: (i, 0)),
                pl.BlockSpec((1, columns), lambda i, t: (0, 0)),
            ],
            out_specs=pl.BlockSpec((per_step * rows, columns), lambda i, t: (i, 0)),
            scratch_shapes=scratch,
        ),
        compiler_params=params(60, ("arbitrary",)),
        name="decode_final",
    )(table, low, own, high, weights, sums, state, gain)


def spread_weights(expand, shrink, gate):
    core = lax.axis_index("seq") % 2
    units = expand.shape[1] // 2
    mine = lax.dynamic_slice_in_dim(expand, core * units, units, 1)
    rows = lax.dynamic_slice_in_dim(shrink, core * units, units, 0)
    cuts = [rows[:, c * units : (c + 1) * units] for c in range(rows.shape[1] // units)]
    pack = jnp.concatenate([mine] + cuts, axis=0)
    count = lax.axis_size("head")
    if count == 4:
        first, second = flipped(pack, 1), flipped(pack, 2)
        half = pack.shape[0] // 2
        _, upper, lower = lax.optimization_barrier((gate, first[:half], second[half:]))
        packs = [[first], [second], [flipped(upper, 2), flipped(lower, 1)]]
    else:
        packs = [[flipped(pack, j)] for j in range(1, count)]
    bands = lax.axis_size("seq")
    pairs = [(i, i ^ 1) for i in range(bands)]
    return packs + [[lax.ppermute(part, "seq", pairs) for part in entry] for entry in packs]


def on_device(
    grid_state,
    encode_index,
    encode_weights,
    first_gain,
    project_in,
    project_out,
    second_gain,
    expand_weights,
    shrink_weights,
    decode_index,
    decode_weights,
    output_gain,
):
    band_number = lax.axis_index("seq")
    band_count = lax.axis_size("seq")
    head_number = lax.axis_index("head")
    head_count = lax.axis_size("head")
    block_rows = encode_weights.shape[2]
    mesh_blocks = encode_weights.shape[0]
    mesh_rows = mesh_blocks * block_rows
    grid_blocks = grid_state.shape[0] // block_rows
    columns = grid_state.shape[1]
    heads_here = columns // HEAD_DIM
    mesh_rim = mesh_blocks // 2
    order = (head_number ^ jnp.arange(head_count, dtype=jnp.int32)).astype(jnp.int32)

    low, high = rims(grid_state, mesh_rows)
    table = (encode_index - (band_number * grid_blocks - mesh_blocks)).reshape(-1)
    mesh_start = encode(table, low, grid_state, high, encode_weights)
    pieces = everyone(mesh_start)

    weight_q = project_in[:, 0].reshape(head_count, columns, columns)
    keys = project_in[:, 1].reshape(D, heads_here // 2, 2, HEAD_DIM)
    values = project_in[:, 2].reshape(D, heads_here // 2, 2, HEAD_DIM)
    weight_kv = jnp.stack(
        [keys[:, :, 0], values[:, :, 0], values[:, :, 1], keys[:, :, 1]], axis=2
    ).reshape(head_count, columns, 2 * columns)
    queries, keys_values = project(
        order, pieces, first_gain.reshape(head_count, 1, columns), weight_q, weight_kv
    )
    low, high = rims(keys_values, min(mesh_rows, WINDOW))

    gate = pieces[-1]
    held = lax.optimization_barrier((gate, project_out))
    whole_out = lax.all_gather(held[1], "head", axis=0, tiled=True)
    packs = spread_weights(expand_weights, shrink_weights, gate)

    share_rows = mesh_rows // head_count
    shares = jnp.stack(
        [
            lax.dynamic_slice_in_dim(p, head_number * share_rows, share_rows, 0)
            for p in pieces
        ]
    )
    start_share = jnp.concatenate([shares[order[i]] for i in range(head_count)], axis=1)

    context = attend(
        (band_number * mesh_rows).astype(jnp.int32).reshape(1),
        mesh_rows * band_count,
        queries,
        low,
        keys_values,
        high,
    )
    context_share = lax.all_to_all(context, "head", split_axis=0, concat_axis=1, tiled=True)
    end_share = feed(
        context_share,
        start_share,
        second_gain.reshape(1, D),
        whole_out,
        expand_weights,
        shrink_weights,
        packs,
    )
    mesh_end = lax.all_to_all(end_share, "head", split_axis=1, concat_axis=0, tiled=True)

    low, high = rims(mesh_end, mesh_rim * block_rows)
    table = (decode_index - (band_number * mesh_blocks - mesh_rim)).reshape(-1)
    sums = decode_sums(table, low, mesh_end, high, decode_weights)
    sums = sum(flipped(sums, j) for j in range(1, head_count)) + sums
    return decode_final(
        table, low, mesh_end, high, decode_weights, sums, grid_state, output_gain.reshape(1, columns)
    )


def solution(mesh):
    return jax.shard_map(
        on_device,
        mesh=mesh,
        in_specs=(
            P("seq", "head"),
            P("seq", None),
            P("seq", None, None, None),
            P(),
            P(None, None, "head"),
            P("head", None),
            P(),
            P(None, "head"),
            P("head", None),
            P("seq", None),
            P("seq", None, None, None),
            P("head"),
        ),
        out_specs=P("seq", "head"),
        check_vma=False,
    )
```
